32 devices in a mesh: dp: 2 (over x), ep: 4 (over z), tp: 4 (over y, core).
Axes of the slice: x: 2, y: 2, z: 4, core: 2. Of those that a mesh axis runs over, the one named last changes fastest.
Arguments:
- X: bfloat16 [4096, 2048], P(('dp', 'ep', 'tp')), parts along dimension 0
- idx: int32 [4096, 8], P(('dp', 'ep', 'tp')), parts along dimension 0
- g: float32 [4096, 8], P(('dp', 'ep', 'tp')), parts along dimension 0
- W1: bfloat16 [64, 2048, 1024], P('ep', None, 'tp')
- W3: bfloat16 [64, 2048, 1024], P('ep', None, 'tp')
- W2: bfloat16 [64, 1024, 2048], P('ep', 'tp')
Outputs:
- output: bfloat16 [4096, 2048], P(('dp', 'ep', 'tp')), parts along dimension 0
There are 2 independent parts. The reference program is written for one: setup_inputs(seed, part) draws one part's arguments, and reference() takes and returns one part's arrays. A program takes and returns all parts, laid end to end along the dimension named above; an argument that names none is the same for every part.
All inputs are finite; a program needn't handle non-finite values.
Results may differ from the reference program's by a relative error of at most 0.0102053.
Values are sent between devices in bfloat16 or wider.
A program may use at most 1 GiB of HBM per device.

```python
import jax
import jax.numpy as jnp
from jax import lax

D = 2048
F = 1024
E = 64
TOP = 8
T_LOC = 128
NDEV = 16
C = 2 * TOP * T_LOC // E
T = NDEV * T_LOC


def _weights(key, shape, fan):
    def one(k):
        return (jax.random.normal(k, shape, jnp.float32) * fan ** -0.5).astype(jnp.bfloat16)
    return lax.map(one, jax.random.split(key, E))


def setup_inputs(seed: int = 0, part: int = 0) -> dict:
    key = jax.random.PRNGKey(seed)
    kdata, kw = jax.random.split(key)
    kx, kr, kg = jax.random.split(jax.random.fold_in(kdata, part), 3)
    k1, k3, k2 = jax.random.split(kw, 3)
    x = jax.random.normal(kx, (T, D), jnp.float32).astype(jnp.bfloat16)
    expert_rank = jnp.arange(E, dtype=jnp.uint32)
    wait_scale = jnp.uint32(512) - (jnp.uint32(256) * expert_rank) // jnp.uint32(max(E - 1, 1))
    wait_time = (jax.random.bits(jax.random.fold_in(kr, 7), (T, E), jnp.uint32) >> 10) * wait_scale[None, :]
    idx = jnp.argsort(wait_time, axis=1)[:, :TOP].astype(jnp.int32)
    g = jax.random.uniform(kg, (T, TOP), jnp.float32, 0.25, 1.0)
    return {"X": x, "idx": idx, "g": g,
            "W1": _weights(k1, (D, F), D), "W3": _weights(k3, (D, F), D), "W2": _weights(k2, (F, D), F)}


def _slots(ids):
    oh = (ids[:, None] == jnp.arange(E, dtype=jnp.int32)[None, :]).astype(jnp.int32)
    return jnp.sum(oh * (jnp.cumsum(oh, axis=0) - 1), axis=1)


def reference(X, idx, g, W1, W3, W2):
    ids = idx.reshape(NDEV, T_LOC * TOP)
    s = jax.vmap(_slots)(ids)
    keep = s < C
    dest = jnp.where(keep, ids * C + s, E * C)
    xr = jnp.repeat(X.reshape(NDEV, T_LOC, D), TOP, axis=1)
    buf = jax.vmap(lambda x, dd: jnp.zeros((E * C, D), X.dtype).at[dd].set(x, mode="drop"))(xr, dest)
    buf = buf.reshape(NDEV, E, C, D).transpose(1, 0, 2, 3)

    def expert(a):
        xb, w1, w3, w2 = a

        def rows(x):
            h1 = jnp.dot(x, w1, preferred_element_type=jnp.float32)
            h3 = jnp.dot(x, w3, preferred_element_type=jnp.float32)
            h = (jax.nn.silu(h1) * h3).astype(jnp.bfloat16)
            return jnp.dot(h, w2, preferred_element_type=jnp.float32).astype(jnp.bfloat16)
        return lax.map(rows, xb)

    yb = lax.map(expert, (buf, W1, W3, W2))
    yb = yb.transpose(1, 0, 2, 3).reshape(NDEV, E * C, D)
    ysel = jax.vmap(lambda y, dd: y[jnp.minimum(dd, E * C - 1)])(yb, dest)
    wgt = jnp.where(keep, g.reshape(NDEV, T_LOC * TOP), 0.0)
    out = jnp.sum(ysel.astype(jnp.float32).reshape(NDEV, T_LOC, TOP, D) * wgt.reshape(NDEV, T_LOC, TOP, 1), axis=2)
    return out.reshape(T, D).astype(jnp.bfloat16)
```

```python
import functools

import jax
import jax.numpy as jnp
from jax import lax
from jax.experimental import pallas as pl
from jax.experimental.pallas import tpu as pltpu
from jax.sharding import PartitionSpec as P

MESH = pl.DeviceIdType.MESH
F32 = jnp.float32
BF16 = jnp.bfloat16

T = 128
HALF = T // 2
TOP = 8
EL = 16
CAP = 32
UNITS = 8
ROWS = UNITS * CAP
NS = 4


def _z_order(z, i):
    inner = (z + 1) // 2 - 2 * (z // 3)
    v = (1 - inner) * (1 + i) + inner * (i + (i + 1) // 2)
    m = z // 2
    return m * (3 - v) + (1 - m) * v


def _r_order(z, i):
    inner = (z + 1) // 2 - 2 * (z // 3)
    odd = i % 2
    v = (1 - inner) * (3 - i) + inner * ((1 - odd) * (3 - i // 2) + odd * (i // 2))
    m = z // 2
    return m * (3 - v) + (1 - m) * v


def _kernel(x_ref, aux_ref, w1_ref, w3_ref, w2_ref, out_ref,
            xall, auxall, xe, w1b, w3b, w2b, spread, tab, pown, dstage, drecv, ystage, yrecv, zstage, zrecv,
            fstage, frecv,
            lsem, lasem, dsem, dasem, ssem, sasem, wsem, rd_s, rd_r, ry_s, ry_r, rz_s, rz_r, rf_s, rf_r):
    d = x_ref.shape[1]
    z = lax.axis_index("ep")
    tp = lax.axis_index("tp")
    y = tp // 2
    c = tp % 2
    me = z * 2 + y
    row0 = pl.multiple_of(c * HALF, HALF)
    oth0 = pl.multiple_of((1 - c) * HALF, HALF)
    mine = pl.ds(row0, HALF)
    amine = pl.ds(pl.multiple_of(c * 8, 8), 8)
    up, down = {"ep": z + 1}, {"ep": z - 1}
    ynbr = {"tp": (1 - y) * 2 + c}
    partner = {"tp": y * 2 + (1 - c)}

    def rcopy(src, dst, s, r, dev):
        return pltpu.make_async_remote_copy(src_ref=src, dst_ref=dst, send_sem=s, recv_sem=r,
                                            device_id=dev, device_id_type=MESH)

    def wcopies(q):
        e, s = q % EL, q % NS
        return (pltpu.make_async_copy(w1_ref.at[e], w1b.at[s], wsem.at[s, 0]),
                pltpu.make_async_copy(w3_ref.at[e], w3b.at[s], wsem.at[s, 1]),
                pltpu.make_async_copy(w2_ref.at[e], w2b.at[s], wsem.at[s, 2]))

    for q in range(NS):
        for cp in wcopies(q):
            cp.start()

    bar = pltpu.get_barrier_semaphore()

    @pl.when(z < 3)
    def _():
        pl.semaphore_signal(bar, inc=1, device_id=up, device_id_type=MESH)

    @pl.when(z > 0)
    def _():
        pl.semaphore_signal(bar, inc=1, device_id=down, device_id_type=MESH)

    pl.semaphore_signal(bar, inc=1, device_id=ynbr, device_id_type=MESH)
    pl.semaphore_signal(bar, inc=1, device_id=partner, device_id_type=MESH)
    inner = (z + 1) // 2 - 2 * (z // 3)
    pl.semaphore_wait(bar, 3 + inner)

    def link_send(h, u, xs, xas, k, dev, op):
        cx = rcopy(xs, xall.at[h, u, mine], ssem.at[h, u, k], lsem.at[h, u], dev)
        ca = rcopy(xas, auxall.at[h, u, amine], sasem.at[h, u, k], lasem.at[h, u], dev)
        if op == "start":
            ca.start()
            cx.start()
        else:
            ca.wait_send()
            cx.wait_send()

    def d2d_send(h, u, op):
        cx = rcopy(xall.at[h, u, mine], xall.at[h, u, mine], ssem.at[h, u, 3], dsem.at[h, u], partner)
        ca = rcopy(auxall.at[h, u, amine], auxall.at[h, u, amine], sasem.at[h, u, 3], dasem.at[h, u], partner)
        if op == "start":
            ca.start()
            cx.start()
        else:
            ca.wait_send()
            cx.wait_send()

    def own_full(h, op):
        cx = rcopy(x_ref, xall.at[h, me], ssem.at[h, me, 3], dsem.at[h, me], partner)
        ca = rcopy(aux_ref, auxall.at[h, me], sasem.at[h, me, 3], dasem.at[h, me], partner)
        if op == "start":
            ca.start()
            cx.start()
        elif op == "send":
            ca.wait_send()
            cx.wait_send()
        else:
            ca.wait_recv()
            cx.wait_recv()

    def own_links(h, xs, xas, op):
        @pl.when(z < 3)
        def _():
            link_send(h, me, xs, xas, 0, up, op)

        @pl.when(z > 0)
        def _():
            link_send(h, me, xs, xas, 1, down, op)

        link_send(h, me, xs, xas, 2, ynbr, op)

    def own_start(h):
        @pl.when(c == h)
        def _():
            own_links(h, x_ref.at[mine], aux_ref.at[amine], "start")
            xall[h, me] = x_ref[...]
            auxall[h, me] = aux_ref[...]

        @pl.when(c != h)
        def _():
            own_full(h, "recv")
            own_links(h, xall.at[h, me, mine], auxall.at[h, me, amine], "start")

    def forwards(h, zz, yy, op):
        u = zz * 2 + yy
        xs, xas = xall.at[h, u, mine], auxall.at[h, u, amine]

        @pl.when(yy == y)
        def _():
            @pl.when(jnp.logical_and(zz < z, z < 3))
            def _():
                link_send(h, u, xs, xas, 0, up, op)

            @pl.when(jnp.logical_and(zz > z, z > 0))
            def _():
                link_send(h, u, xs, xas, 1, down, op)

            link_send(h, u, xs, xas, 2, ynbr, op)

        d2d_send(h, u, op)

    def piece(k):
        along_z = (1 - k % 2) * (1 - k // 6)
        i = k // 2
        first = 1 - (i + 2) // 3
        zi = _z_order(z, i - i // 3)
        zy = first * z + (1 - first) * _z_order(z, (i - 1) * (1 - first))
        zz = along_z * zi + (1 - along_z) * zy
        yy = along_z * y + (1 - along_z) * (1 - y)
        return zz, yy

    def ag_step(h, k):
        zz, yy = piece(k)
        u = zz * 2 + yy
        rcopy(auxall.at[h, u, amine], auxall.at[h, u, amine], sasem.at[h, u, 0], lasem.at[h, u], partner).wait_recv()
        rcopy(xall.at[h, u, mine], xall.at[h, u, mine], ssem.at[h, u, 0], lsem.at[h, u], partner).wait_recv()
        forwards(h, zz, yy, "start")

    def d2d_wait(h, k):
        zz, yy = piece(k)
        u = zz * 2 + yy
        oth = pl.ds(oth0, HALF)
        aoth = pl.ds(pl.multiple_of((1 - c) * 8, 8), 8)
        rcopy(auxall.at[h, u, aoth], auxall.at[h, u, aoth], sasem.at[h, u, 0], dasem.at[h, u], partner).wait_recv()
        rcopy(xall.at[h, u, oth], xall.at[h, u, oth], ssem.at[h, u, 0], dsem.at[h, u], partner).wait_recv()
        return u

    lane = lax.broadcasted_iota(jnp.int32, (T, 4 * EL * CAP), 1)
    sub = lax.broadcasted_iota(jnp.int32, (T, 4 * EL * CAP), 0)
    spread[...] = jnp.where(lane // CAP == sub, 1.0, 0.0).astype(BF16)

    def gather(h, u):
        aux = auxall[h, u]
        eg = (lax.broadcasted_iota(jnp.int32, (EL, T), 0) + z * EL).astype(F32)
        hit = jnp.zeros((EL, T), F32)
        gate = jnp.zeros((EL, T), F32)
        for j in range(TOP):
            eq = aux[j:j + 1, :] == eg
            hit = jnp.where(eq, 1.0, hit)
            gate = jnp.where(eq, aux[TOP + j:TOP + j + 1, :], gate)
        before = lax.broadcasted_iota(jnp.int32, (T, T), 0) < lax.broadcasted_iota(jnp.int32, (T, T), 1)
        tri = jnp.where(before, 1.0, 0.0).astype(BF16)
        slot = jnp.dot(hit.astype(BF16), tri, preferred_element_type=F32)
        keep = jnp.logical_and(hit > 0.5, slot < CAP - 0.5)
        slot = jnp.where(keep, slot, -1.0)
        g1 = gate.astype(BF16).astype(F32)
        r1 = gate - g1
        g2 = r1.astype(BF16).astype(F32)
        g3 = r1 - g2
        stack = jnp.concatenate([slot, g1, g2, g3, jnp.zeros((T - 4 * EL, T), F32)], axis=0)
        tab[h, u] = stack.T.astype(BF16)
        pos = lax.broadcasted_iota(jnp.int32, (EL, CAP, T), 1).astype(F32)
        hot = jnp.where(slot[:, None, :] == pos, 1.0, 0.0).reshape(EL * CAP, T).astype(BF16)
        rows = pl.ds(pl.multiple_of(u * CAP, CAP), CAP)
        for n in range(0, d, 512):
            xg = jnp.dot(hot, xall[h, u, :, n:n + 512], preferred_element_type=F32).astype(BF16)
            xe[:, rows, n:n + 512] = xg.reshape(EL, CAP, 512)

    def expert(q):
        e, s = q % EL, q % NS
        c1, c3, c2 = wcopies(q)
        c1.wait()
        a = jnp.dot(xe[e], w1b[s], preferred_element_type=F32)
        c3.wait()
        b = jnp.dot(xe[e], w3b[s], preferred_element_type=F32)
        hh = (a * jax.nn.sigmoid(a) * b).astype(BF16)
        c2.wait()
        for n in range(0, d, 512):
            xe[e, :, n:n + 512] = jnp.dot(hh, w2b[s, :, n:n + 512], preferred_element_type=F32).astype(BF16)

        @pl.when(q + NS < 2 * EL)
        def _():
            for cp in wcopies(q + NS):
                cp.start()

    slots_of = (lax.broadcasted_iota(jnp.int32, (T, EL * CAP), 1) % CAP).astype(F32)

    def dcopy(h, u):
        return rcopy(dstage.at[u], drecv.at[h, u], rd_s.at[h, u], rd_r.at[h, u], partner)

    def ycopy(h, zz):
        return rcopy(ystage.at[zz], yrecv.at[h, zz], ry_s.at[h, zz], ry_r.at[h, zz], ynbr)

    def zcopy(h, zz, slot, dev):
        return rcopy(zstage.at[zz], zrecv.at[h, slot], rz_s.at[h, zz], rz_r.at[h, slot], dev)

    def fcopy():
        return rcopy(fstage, frecv, rf_s, rf_r, partner)

    def combine(h, u):
        tb = jnp.concatenate([tab[h, u, mine], tab[h, u, pl.ds(oth0, HALF)]], axis=0)
        ex = jnp.dot(tb, spread[...], preferred_element_type=F32)
        n0 = EL * CAP
        on = ex[:, :n0] == slots_of
        lhs = jnp.concatenate([jnp.where(on, ex[:, k * n0:(k + 1) * n0], 0.0).astype(BF16) for k in (1, 2, 3)], axis=0)
        rows = pl.ds(pl.multiple_of(u * CAP, CAP), CAP)
        if h == 1:
            dcopy(0, u).wait_send()
        for n in range(0, d, 512):
            yy = xe[:, rows, n:n + 512].reshape(EL * CAP, 512)
            p3 = jnp.dot(lhs, yy, preferred_element_type=F32)
            p = p3[:T] + p3[T:2 * T] + p3[2 * T:]
            pown[u, :, n:n + 512] = p[:HALF]
            dstage[u, :, n:n + 512] = p[HALF:].astype(BF16)
        dcopy(h, u).start()

    def fin_y(h, i):
        zz = _r_order(z, i)
        u = zz * 2 + (1 - y)
        dcopy(h, u).wait_recv()
        if h == 1:
            ycopy(0, zz).wait_send()
        ystage[zz] = (pown[u] + drecv[h, u].astype(F32)).astype(BF16)
        ycopy(h, zz).start()

    def fin_z(h, i):
        zz = _r_order(z, i)
        u = zz * 2 + y
        dcopy(h, u).wait_recv()
        ycopy(h, zz).wait_recv()

        @pl.when(jnp.logical_or(jnp.logical_and(zz > z, z > 0), jnp.logical_and(zz < z, z < 3)))
        def _():
            zcopy(h, zz, zz, up).wait_recv()
            pown[u] = pown[u] + zrecv[h, zz].astype(F32)

        if h == 1:
            zcopy(0, zz, zz, up).wait_send()
        zstage[zz] = (pown[u] + drecv[h, u].astype(F32) + yrecv[h, zz].astype(F32)).astype(BF16)

        @pl.when(zz == z + 1)
        def _():
            zcopy(h, zz, 4, up).start()

        @pl.when(zz > z + 1)
        def _():
            zcopy(h, zz, zz, up).start()

        @pl.when(zz < z)
        def _():
            zcopy(h, zz, zz, down).start()

    def fin_own(h):
        u = me
        dcopy(h, u).wait_recv()
        ycopy(h, z).wait_recv()
        pown[u] = pown[u] + drecv[h, u].astype(F32) + yrecv[h, z].astype(F32)

        @pl.when(z < 3)
        def _():
            zcopy(h, z, z, up).wait_recv()
            pown[u] = pown[u] + zrecv[h, z].astype(F32)

        @pl.when(z > 0)
        def _():
            zcopy(h, z, 4, up).wait_recv()
            pown[u] = pown[u] + zrecv[h, 4].astype(F32)

        @pl.when(c == h)
        def _():
            out_ref[mine, :] = pown[u].astype(BF16)

        @pl.when(c != h)
        def _():
            fstage[...] = pown[u].astype(BF16)
            fcopy().start()

    for h in range(2):
        @pl.when(c == h)
        def _():
            own_full(h, "start")
    own_start(0)
    gather(0, me)

    def a_body(k, _):
        @pl.when(k < 7)
        def _():
            ag_step(0, k)

        @pl.when(k == 4)
        def _():
            own_start(1)

        @pl.when(k > 0)
        def _():
            gather(0, d2d_wait(0, k - 1))
        return 0

    lax.fori_loop(0, 8, a_body, 0)

    def ffn_a(e, _):
        expert(e)
        for k, at in enumerate((4, 5, 9, 10, 14, 15)):
            @pl.when(e == at)
            def _():
                ag_step(1, k)
        return 0

    lax.fori_loop(0, EL, ffn_a, 0)

    def comb_all(h):
        def body(i, _):
            yy = (1 - i // 4) * (1 - y) + (i // 4) * y
            combine(h, _r_order(z, i % 4) * 2 + yy)

            @pl.when(jnp.logical_and(i > 0, i < 5))
            def _():
                fin_y(h, i - 1)
            if h == 0:
                @pl.when(i == 3)
                def _():
                    ag_step(1, 6)
            return 0
        lax.fori_loop(0, 8, body, 0)

    comb_all(0)

    def b_body(k, _):
        @pl.when(k == 0)
        def _():
            gather(1, me)

        @pl.when(k > 0)
        def _():
            gather(1, d2d_wait(1, k - 1))
        return 0

    lax.fori_loop(0, 8, b_body, 0)

    def ffn_b(e, _):
        expert(EL + e)
        for i in range(3):
            @pl.when(e == 4 * i + 1 + 4 * inner)
            def _():
                fin_z(0, i)
        return 0

    lax.fori_loop(0, EL, ffn_b, 0)
    fin_own(0)
    comb_all(1)

    def last_z(i, _):
        fin_z(1, i)
        return 0

    lax.fori_loop(0, 3, last_z, 0)
    fin_own(1)

    fcopy().wait_recv()
    out_ref[pl.ds(oth0, HALF), :] = frecv[...]

    fcopy().wait_send()
    for h in range(2):
        @pl.when(c == h)
        def _():
            own_full(h, "send")
        own_links(h, xall.at[h, me, mine], auxall.at[h, me, amine], "send")

        def drain(k, _):
            zz, yy = piece(k)
            forwards(h, zz, yy, "send")
            return 0
        lax.fori_loop(0, 7, drain, 0)

    def drain_r(i, _):
        zz = _r_order(z, i)
        dcopy(1, zz * 2).wait_send()
        dcopy(1, zz * 2 + 1).wait_send()
        ycopy(1, zz).wait_send()

        @pl.when(i < 3)
        def _():
            zcopy(1, zz, zz, up).wait_send()
        return 0
    lax.fori_loop(0, 4, drain_r, 0)


def solution(mesh):
    rows = P(("dp", "ep", "tp"), None)

    def local(x, idx, g, w1, w3, w2):
        d = x.shape[1]
        f = w1.shape[2]
        aux = jnp.concatenate([idx.T.astype(F32), g.T], axis=0)
        vm = pl.BlockSpec(memory_space=pltpu.VMEM)
        hbm = pl.BlockSpec(memory_space=pl.ANY)
        dma = pltpu.SemaphoreType.DMA
        return pl.pallas_call(
            _kernel,
            out_shape=jax.ShapeDtypeStruct((T, d), BF16),
            in_specs=[vm, vm, hbm, hbm, hbm],
            out_specs=vm,
            scratch_shapes=[
                pltpu.VMEM((2, UNITS, T, d), BF16),
                pltpu.VMEM((2, UNITS, 2 * TOP, T), F32),
                pltpu.VMEM((EL, ROWS, d), BF16),
                pltpu.VMEM((NS, d, f), BF16),
                pltpu.VMEM((NS, d, f), BF16),
                pltpu.VMEM((NS, f, d), BF16),
                pltpu.VMEM((T, 4 * EL * CAP), BF16),
                pltpu.VMEM((2, UNITS, T, T), BF16),
                pltpu.VMEM((UNITS, HALF, d), F32),
                pltpu.VMEM((UNITS, HALF, d), BF16),
                pltpu.VMEM((2, UNITS, HALF, d), BF16),
                pltpu.VMEM((4, HALF, d), BF16),
                pltpu.VMEM((2, 4, HALF, d), BF16),
                pltpu.VMEM((4, HALF, d), BF16),
                pltpu.VMEM((2, 5, HALF, d), BF16),
                pltpu.VMEM((HALF, d), BF16),
                pltpu.VMEM((HALF, d), BF16),
                dma((2, UNITS)), dma((2, UNITS)), dma((2, UNITS)), dma((2, UNITS)),
                dma((2, UNITS, 4)), dma((2, UNITS, 4)),
                dma((NS, 3)),
                dma((2, UNITS)), dma((2, UNITS)),
                dma((2, 4)), dma((2, 4)),
                dma((2, 4)), dma((2, 5)),
                dma, dma,
            ],
            compiler_params=pltpu.CompilerParams(collective_id=0, has_side_effects=True,
                                                 vmem_limit_bytes=67043328),
        )(x, aux, w1, w3, w2)

    return jax.shard_map(local, mesh=mesh,
                         in_specs=(rows, rows, rows, P("ep", None, "tp"), P("ep", None, "tp"), P("ep", "tp", None)),
                         out_specs=rows, check_vma=False)
```

```python
import functools

import jax
import jax.numpy as jnp
from jax import lax
from jax.experimental import pallas as pl
from jax.experimental.pallas import tpu as pltpu
from jax.sharding import PartitionSpec as P

MESH = pl.DeviceIdType.MESH
F32 = jnp.float32
BF16 = jnp.bfloat16

T = 128
HALF = T // 2
TOP = 8
EL = 16
CAP = 32
UNITS = 8
ROWS = UNITS * CAP
NS = 4


def _z_order(z, i):
    inner = (z + 1) // 2 - 2 * (z // 3)
    v = (1 - inner) * (1 + i) + inner * (i + (i + 1) // 2)
    m = z // 2
    return m * (3 - v) + (1 - m) * v


def _r_order(z, i):
    inner = (z + 1) // 2 - 2 * (z // 3)
    odd = i % 2
    v = (1 - inner) * (3 - i) + inner * ((1 - odd) * (3 - i // 2) + odd * (i // 2))
    m = z // 2
    return m * (3 - v) + (1 - m) * v


def _kernel(x_ref, aux_ref, w1_ref, w3_ref, w2_ref, out_ref,
            xall, auxall, xe, w1b, w3b, w2b, spread, tab, pown, dstage, drecv, ystage, yrecv, zstage, zrecv,
            fstage, frecv,
            lsem, lasem, dsem, dasem, ssem, sasem, wsem, rd_s, rd_r, ry_s, ry_r, rz_s, rz_r, rf_s, rf_r):
    d = x_ref.shape[1]
    z = lax.axis_index("ep")
    tp = lax.axis_index("tp")
    y = tp // 2
    c = tp % 2
    me = z * 2 + y
    row0 = pl.multiple_of(c * HALF, HALF)
    oth0 = pl.multiple_of((1 - c) * HALF, HALF)
    mine = pl.ds(row0, HALF)
    amine = pl.ds(pl.multiple_of(c * 8, 8), 8)
    up, down = {"ep": z + 1}, {"ep": z - 1}
    ynbr = {"tp": (1 - y) * 2 + c}
    partner = {"tp": y * 2 + (1 - c)}

    def rcopy(src, dst, s, r, dev):
        return pltpu.make_async_remote_copy(src_ref=src, dst_ref=dst, send_sem=s, recv_sem=r,
                                            device_id=dev, device_id_type=MESH)

    def wcopies(q):
        e, s = q % EL, q % NS
        return (pltpu.make_async_copy(w1_ref.at[e], w1b.at[s], wsem.at[s, 0]),
                pltpu.make_async_copy(w3_ref.at[e], w3b.at[s], wsem.at[s, 1]),
                pltpu.make_async_copy(w2_ref.at[e], w2b.at[s], wsem.at[s, 2]))

    for q in range(NS):
        for cp in wcopies(q):
            cp.start()

    bar = pltpu.get_barrier_semaphore()

    @pl.when(z < 3)
    def _():
        pl.semaphore_signal(bar, inc=1, device_id=up, device_id_type=MESH)

    @pl.when(z > 0)
    def _():
        pl.semaphore_signal(bar, inc=1, device_id=down, device_id_type=MESH)

    pl.semaphore_signal(bar, inc=1, device_id=ynbr, device_id_type=MESH)
    pl.semaphore_signal(bar, inc=1, device_id=partner, device_id_type=MESH)
    inner = (z + 1) // 2 - 2 * (z // 3)
    pl.semaphore_wait(bar, 3 + inner)

    def link_send(h, u, xs, xas, k, dev, op):
        cx = rcopy(xs, xall.at[h, u, mine], ssem.at[h, u, k], lsem.at[h, u], dev)
        ca = rcopy(xas, auxall.at[h, u, amine], sasem.at[h, u, k], lasem.at[h, u], dev)
        if op == "start":
            ca.start()
            cx.start()
        else:
            ca.wait_send()
            cx.wait_send()

    def d2d_send(h, u, op):
        cx = rcopy(xall.at[h, u, mine], xall.at[h, u, mine], ssem.at[h, u, 3], dsem.at[h, u], partner)
        ca = rcopy(auxall.at[h, u, amine], auxall.at[h, u, amine], sasem.at[h, u, 3], dasem.at[h, u], partner)
        if op == "start":
            ca.start()
            cx.start()
        else:
            ca.wait_send()
            cx.wait_send()

    def own_full(h, op):
        cx = rcopy(x_ref, xall.at[h, me], ssem.at[h, me, 3], dsem.at[h, me], partner)
        ca = rcopy(aux_ref, auxall.at[h, me], sasem.at[h, me, 3], dasem.at[h, me], partner)
        if op == "start":
            ca.start()
            cx.start()
        elif op == "send":
            ca.wait_send()
            cx.wait_send()
        else:
            ca.wait_recv()
            cx.wait_recv()

    def own_links(h, xs, xas, op):
        @pl.when(z < 3)
        def _():
            link_send(h, me, xs, xas, 0, up, op)

        @pl.when(z > 0)
        def _():
            link_send(h, me, xs, xas, 1, down, op)

        link_send(h, me, xs, xas, 2, ynbr, op)

    def own_start(h):
        @pl.when(c == h)
        def _():
            own_links(h, x_ref.at[mine], aux_ref.at[amine], "start")
            xall[h, me] = x_ref[...]
            auxall[h, me] = aux_ref[...]

        @pl.when(c != h)
        def _():
            own_full(h, "recv")
            own_links(h, xall.at[h, me, mine], auxall.at[h, me, amine], "start")

    def forwards(h, zz, yy, op):
        u = zz * 2 + yy
        xs, xas = xall.at[h, u, mine], auxall.at[h, u, amine]

        @pl.when(yy == y)
        def _():
            @pl.when(jnp.logical_and(zz < z, z < 3))
            def _():
                link_send(h, u, xs, xas, 0, up, op)

            @pl.when(jnp.logical_and(zz > z, z > 0))
            def _():
                link_send(h, u, xs, xas, 1, down, op)

            link_send(h, u, xs, xas, 2, ynbr, op)

        d2d_send(h, u, op)

    def piece(k):
        along_z = (1 - k % 2) * (1 - k // 6)
        i = k // 2
        first = 1 - (i + 2) // 3
        zi = _z_order(z, i - i // 3)
        zy = first * z + (1 - first) * _z_order(z, (i - 1) * (1 - first))
        zz = along_z * zi + (1 - along_z) * zy
        yy = along_z * y + (1 - along_z) * (1 - y)
        return zz, yy

    def ag_step(h, k):
        zz, yy = piece(k)
        u = zz * 2 + yy
        rcopy(auxall.at[h, u, amine], auxall.at[h, u, amine], sasem.at[h, u, 0], lasem.at[h, u], partner).wait_recv()
        rcopy(xall.at[h, u, mine], xall.at[h, u, mine], ssem.at[h, u, 0], lsem.at[h, u], partner).wait_recv()
        forwards(h, zz, yy, "start")

    def d2d_wait(h, k):
        zz, yy = piece(k)
        u = zz * 2 + yy
        oth = pl.ds(oth0, HALF)
        aoth = pl.ds(pl.multiple_of((1 - c) * 8, 8), 8)
        rcopy(auxall.at[h, u, aoth], auxall.at[h, u, aoth], sasem.at[h, u, 0], dasem.at[h, u], partner).wait_recv()
        rcopy(xall.at[h, u, oth], xall.at[h, u, oth], ssem.at[h, u, 0], dsem.at[h, u], partner).wait_recv()
        return u

    lane = lax.broadcasted_iota(jnp.int32, (T, 4 * EL * CAP), 1)
    sub = lax.broadcasted_iota(jnp.int32, (T, 4 * EL * CAP), 0)
    spread[...] = jnp.where(lane // CAP == sub, 1.0, 0.0).astype(BF16)

    def gather(h, u):
        aux = auxall[h, u]
        eg = (lax.broadcasted_iota(jnp.int32, (EL, T), 0) + z * EL).astype(F32)
        hit = jnp.zeros((EL, T), F32)
        gate = jnp.zeros((EL, T), F32)
        for j in range(TOP):
            eq = aux[j:j + 1, :] == eg
            hit = jnp.where(eq, 1.0, hit)
            gate = jnp.where(eq, aux[TOP + j:TOP + j + 1, :], gate)
        before = lax.broadcasted_iota(jnp.int32, (T, T), 0) < lax.broadcasted_iota(jnp.int32, (T, T), 1)
        tri = jnp.where(before, 1.0, 0.0).astype(BF16)
        slot = jnp.dot(hit.astype(BF16), tri, preferred_element_type=F32)
        keep = jnp.logical_and(hit > 0.5, slot < CAP - 0.5)
        slot = jnp.where(keep, slot, -1.0)
        g1 = gate.astype(BF16).astype(F32)
        r1 = gate - g1
        g2 = r1.astype(BF16).astype(F32)
        g3 = r1 - g2
        stack = jnp.concatenate([slot, g1, g2, g3, jnp.zeros((T - 4 * EL, T), F32)], axis=0)
        tab[h, u] = stack.T.astype(BF16)
        pos = lax.broadcasted_iota(jnp.int32, (EL, CAP, T), 1).astype(F32)
        hot = jnp.where(slot[:, None, :] == pos, 1.0, 0.0).reshape(EL * CAP, T).astype(BF16)
        rows = pl.ds(pl.multiple_of(u * CAP, CAP), CAP)
        for n in range(0, d, 512):
            xg = jnp.dot(hot, xall[h, u, :, n:n + 512], preferred_element_type=F32).astype(BF16)
            xe[:, rows, n:n + 512] = xg.reshape(EL, CAP, 512)

    def expert(q):
        e, s = q % EL, q % NS
        c1, c3, c2 = wcopies(q)
        c1.wait()
        c3.wait()
        c2.wait()
        a = jnp.dot(xe[e], w1b[s], preferred_element_type=F32)
        b = jnp.dot(xe[e], w3b[s], preferred_element_type=F32)
        hh = (a * jax.nn.sigmoid(a) * b).astype(BF16)
        for n in range(0, d, 512):
            xe[e, :, n:n + 512] = jnp.dot(hh, w2b[s, :, n:n + 512], preferred_element_type=F32).astype(BF16)

        @pl.when(q + NS < 2 * EL)
        def _():
            for cp in wcopies(q + NS):
                cp.start()

    slots_of = (lax.broadcasted_iota(jnp.int32, (T, EL * CAP), 1) % CAP).astype(F32)

    def dcopy(h, u):
        return rcopy(dstage.at[u], drecv.at[h, u], rd_s.at[h, u], rd_r.at[h, u], partner)

    def ycopy(h, zz):
        return rcopy(ystage.at[zz], yrecv.at[h, zz], ry_s.at[h, zz], ry_r.at[h, zz], ynbr)

    def zcopy(h, zz, slot, dev):
        return rcopy(zstage.at[zz], zrecv.at[h, slot], rz_s.at[h, zz], rz_r.at[h, slot], dev)

    def fcopy():
        return rcopy(fstage, frecv, rf_s, rf_r, partner)

    def combine(h, u):
        tb = jnp.concatenate([tab[h, u, mine], tab[h, u, pl.ds(oth0, HALF)]], axis=0)
        ex = jnp.dot(tb, spread[...], preferred_element_type=F32)
        n0 = EL * CAP
        on = ex[:, :n0] == slots_of
        lhs = jnp.concatenate([jnp.where(on, ex[:, k * n0:(k + 1) * n0], 0.0).astype(BF16) for k in (1, 2, 3)], axis=0)
        rows = pl.ds(pl.multiple_of(u * CAP, CAP), CAP)
        if h == 1:
            dcopy(0, u).wait_send()
        for n in range(0, d, 512):
            yy = xe[:, rows, n:n + 512].reshape(EL * CAP, 512)
            p3 = jnp.dot(lhs, yy, preferred_element_type=F32)
            p = p3[:T] + p3[T:2 * T] + p3[2 * T:]
            pown[u, :, n:n + 512] = p[:HALF]
            dstage[u, :, n:n + 512] = p[HALF:].astype(BF16)
        dcopy(h, u).start()

    def fin_y(h, i):
        zz = _r_order(z, i)
        u = zz * 2 + (1 - y)
        dcopy(h, u).wait_recv()
        if h == 1:
            ycopy(0, zz).wait_send()
        ystage[zz] = (pown[u] + drecv[h, u].astype(F32)).astype(BF16)
        ycopy(h, zz).start()

    def fin_z(h, i):
        zz = _r_order(z, i)
        u = zz * 2 + y
        dcopy(h, u).wait_recv()
        ycopy(h, zz).wait_recv()

        @pl.when(jnp.logical_or(jnp.logical_and(zz > z, z > 0), jnp.logical_and(zz < z, z < 3)))
        def _():
            zcopy(h, zz, zz, up).wait_recv()
            pown[u] = pown[u] + zrecv[h, zz].astype(F32)

        if h == 1:
            zcopy(0, zz, zz, up).wait_send()
        zstage[zz] = (pown[u] + drecv[h, u].astype(F32) + yrecv[h, zz].astype(F32)).astype(BF16)

        @pl.when(zz == z + 1)
        def _():
            zcopy(h, zz, 4, up).start()

        @pl.when(zz > z + 1)
        def _():
            zcopy(h, zz, zz, up).start()

        @pl.when(zz < z)
        def _():
            zcopy(h, zz, zz, down).start()

    def fin_own(h):
        u = me
        dcopy(h, u).wait_recv()
        ycopy(h, z).wait_recv()
        pown[u] = pown[u] + drecv[h, u].astype(F32) + yrecv[h, z].astype(F32)

        @pl.when(z < 3)
        def _():
            zcopy(h, z, z, up).wait_recv()
            pown[u] = pown[u] + zrecv[h, z].astype(F32)

        @pl.when(z > 0)
        def _():
            zcopy(h, z, 4, up).wait_recv()
            pown[u] = pown[u] + zrecv[h, 4].astype(F32)

        @pl.when(c == h)
        def _():
            out_ref[mine, :] = pown[u].astype(BF16)

        @pl.when(c != h)
        def _():
            fstage[...] = pown[u].astype(BF16)
            fcopy().start()

    for h in range(2):
        @pl.when(c == h)
        def _():
            own_full(h, "start")
    own_start(0)
    gather(0, me)

    def a_body(k, _):
        @pl.when(k < 7)
        def _():
            ag_step(0, k)

        @pl.when(k == 4)
        def _():
            own_start(1)

        @pl.when(k > 0)
        def _():
            gather(0, d2d_wait(0, k - 1))
        return 0

    lax.fori_loop(0, 8, a_body, 0)

    def ffn_a(e, _):
        expert(e)
        for k, at in enumerate((4, 5, 9, 10, 14, 15)):
            @pl.when(e == at)
            def _():
                ag_step(1, k)
        return 0

    lax.fori_loop(0, EL, ffn_a, 0)

    def comb_all(h):
        def body(i, _):
            yy = (1 - i // 4) * (1 - y) + (i // 4) * y
            combine(h, _r_order(z, i % 4) * 2 + yy)

            @pl.when(jnp.logical_and(i > 0, i < 5))
            def _():
                fin_y(h, i - 1)
            if h == 0:
                @pl.when(i == 3)
                def _():
                    ag_step(1, 6)
            return 0
        lax.fori_loop(0, 8, body, 0)

    comb_all(0)

    def b_body(k, _):
        @pl.when(k == 0)
        def _():
            gather(1, me)

        @pl.when(k > 0)
        def _():
            gather(1, d2d_wait(1, k - 1))
        return 0

    lax.fori_loop(0, 8, b_body, 0)

    def ffn_b(e, _):
        expert(EL + e)
        for i in range(3):
            @pl.when(e == 4 * i + 1 + 4 * inner)
            def _():
                fin_z(0, i)
        return 0

    lax.fori_loop(0, EL, ffn_b, 0)
    fin_own(0)
    comb_all(1)

    def last_z(i, _):
        fin_z(1, i)
        return 0

    lax.fori_loop(0, 3, last_z, 0)
    fin_own(1)

    fcopy().wait_recv()
    out_ref[pl.ds(oth0, HALF), :] = frecv[...]

    fcopy().wait_send()
    for h in range(2):
        @pl.when(c == h)
        def _():
            own_full(h, "send")
        own_links(h, xall.at[h, me, mine], auxall.at[h, me, amine], "send")

        def drain(k, _):
            zz, yy = piece(k)
            forwards(h, zz, yy, "send")
            return 0
        lax.fori_loop(0, 7, drain, 0)

    def drain_r(i, _):
        zz = _r_order(z, i)
        dcopy(1, zz * 2).wait_send()
        dcopy(1, zz * 2 + 1).wait_send()
        ycopy(1, zz).wait_send()

        @pl.when(i < 3)
        def _():
            zcopy(1, zz, zz, up).wait_send()
        return 0
    lax.fori_loop(0, 4, drain_r, 0)


def solution(mesh):
    rows = P(("dp", "ep", "tp"), None)

    def local(x, idx, g, w1, w3, w2):
        d = x.shape[1]
        f = w1.shape[2]
        aux = jnp.concatenate([idx.T.astype(F32), g.T], axis=0)
        vm = pl.BlockSpec(memory_space=pltpu.VMEM)
        hbm = pl.BlockSpec(memory_space=pl.ANY)
        dma = pltpu.SemaphoreType.DMA
        return pl.pallas_call(
            _kernel,
            out_shape=jax.ShapeDtypeStruct((T, d), BF16),
            in_specs=[vm, vm, hbm, hbm, hbm],
            out_specs=vm,
            scratch_shapes=[
                pltpu.VMEM((2, UNITS, T, d), BF16),
                pltpu.VMEM((2, UNITS, 2 * TOP, T), F32),
                pltpu.VMEM((EL, ROWS, d), BF16),
                pltpu.VMEM((NS, d, f), BF16),
                pltpu.VMEM((NS, d, f), BF16),
                pltpu.VMEM((NS, f, d), BF16),
                pltpu.VMEM((T, 4 * EL * CAP), BF16),
                pltpu.VMEM((2, UNITS, T, T), BF16),
                pltpu.VMEM((UNITS, HALF, d), F32),
                pltpu.VMEM((UNITS, HALF, d), BF16),
                pltpu.VMEM((2, UNITS, HALF, d), BF16),
                pltpu.VMEM((4, HALF, d), BF16),
                pltpu.VMEM((2, 4, HALF, d), BF16),
                pltpu.VMEM((4, HALF, d), BF16),
                pltpu.VMEM((2, 5, HALF, d), BF16),
                pltpu.VMEM((HALF, d), BF16),
                pltpu.VMEM((HALF, d), BF16),
                dma((2, UNITS)), dma((2, UNITS)), dma((2, UNITS)), dma((2, UNITS)),
                dma((2, UNITS, 4)), dma((2, UNITS, 4)),
                dma((NS, 3)),
                dma((2, UNITS)), dma((2, UNITS)),
                dma((2, 4)), dma((2, 4)),
                dma((2, 4)), dma((2, 5)),
                dma, dma,
            ],
            compiler_params=pltpu.CompilerParams(collective_id=0, has_side_effects=True,
                                                 vmem_limit_bytes=67043328),
        )(x, aux, w1, w3, w2)

    return jax.shard_map(local, mesh=mesh,
                         in_specs=(rows, rows, rows, P("ep", None, "tp"), P("ep", None, "tp"), P("ep", "tp", None)),
                         out_specs=rows, check_vma=False)
```

```python
import functools

import jax
import jax.numpy as jnp
from jax import lax
from jax.experimental import pallas as pl
from jax.experimental.pallas import tpu as pltpu
from jax.sharding import PartitionSpec as P

MESH = pl.DeviceIdType.MESH
F32 = jnp.float32
BF16 = jnp.bfloat16

T = 128
HALF = T // 2
PART = HALF // 2
TOP = 8
EL = 16
CAP = 32
UNITS = 8
ROWS = UNITS * CAP
NS = 4


def _z_order(z, i):
    inner = (z + 1) // 2 - 2 * (z // 3)
    v = (1 - inner) * (1 + i) + inner * (i + (i + 1) // 2)
    m = z // 2
    return m * (3 - v) + (1 - m) * v


def _r_order(z, i):
    inner = (z + 1) // 2 - 2 * (z // 3)
    odd = i % 2
    v = (1 - inner) * (3 - i) + inner * ((1 - odd) * (3 - i // 2) + odd * (i // 2))
    m = z // 2
    return m * (3 - v) + (1 - m) * v


def _kernel(x_ref, aux_ref, w1_ref, w3_ref, w2_ref, out_ref,
            xall, auxall, xe, w1b, w3b, w2b, spread, tab, pown, dstage, drecv, ystage, yrecv, zstage, zrecv,
            fstage, frecv, astage, arecv,
            lsem, lasem, dsem, dasem, ssem, sasem, wsem, rd_s, rd_r, ry_s, ry_r, rz_s, rz_r, ra_s, ra_r, rf_s, rf_r):
    d = x_ref.shape[1]
    z = lax.axis_index("ep")
    tp = lax.axis_index("tp")
    y = tp // 2
    c = tp % 2
    me = z * 2 + y
    pz = z + 1 - 2 * (z % 2)
    row0 = pl.multiple_of(c * HALF, HALF)
    oth0 = pl.multiple_of((1 - c) * HALF, HALF)
    mine = pl.ds(row0, HALF)
    amine = pl.ds(pl.multiple_of(c * 8, 8), 8)
    up, down = {"ep": z + 1}, {"ep": z - 1}
    ynbr = {"tp": (1 - y) * 2 + c}
    partner = {"tp": y * 2 + (1 - c)}

    def rcopy(src, dst, s, r, dev):
        return pltpu.make_async_remote_copy(src_ref=src, dst_ref=dst, send_sem=s, recv_sem=r,
                                            device_id=dev, device_id_type=MESH)

    def wcopies(q):
        e, s = q % EL, q % NS
        return (pltpu.make_async_copy(w1_ref.at[e], w1b.at[s], wsem.at[s, 0]),
                pltpu.make_async_copy(w3_ref.at[e], w3b.at[s], wsem.at[s, 1]),
                pltpu.make_async_copy(w2_ref.at[e], w2b.at[s], wsem.at[s, 2]))

    for q in range(NS):
        for cp in wcopies(q):
            cp.start()

    bar = pltpu.get_barrier_semaphore()

    @pl.when(z < 3)
    def _():
        pl.semaphore_signal(bar, inc=1, device_id=up, device_id_type=MESH)

    @pl.when(z > 0)
    def _():
        pl.semaphore_signal(bar, inc=1, device_id=down, device_id_type=MESH)

    pl.semaphore_signal(bar, inc=1, device_id=ynbr, device_id_type=MESH)
    pl.semaphore_signal(bar, inc=1, device_id=partner, device_id_type=MESH)
    inner = (z + 1) // 2 - 2 * (z // 3)
    pl.semaphore_wait(bar, 3 + inner)

    def part(r0, p):
        return pl.ds(pl.multiple_of(r0 + p * PART, PART), PART)

    def link_send(h, u, p, k, dev, op, xs=None, xas=None):
        xs = xall.at[h, u, part(row0, p)] if xs is None else xs
        cx = rcopy(xs, xall.at[h, u, part(row0, p)], ssem.at[h, u, p, k], lsem.at[h, u, p], dev)
        if p == 0:
            xas = auxall.at[h, u, amine] if xas is None else xas
            ca = rcopy(xas, auxall.at[h, u, amine], sasem.at[h, u, k], lasem.at[h, u], dev)
            ca.start() if op == "start" else ca.wait_send()
        cx.start() if op == "start" else cx.wait_send()

    def d2d_send(h, u, p, op):
        cx = rcopy(xall.at[h, u, part(row0, p)], xall.at[h, u, part(row0, p)], ssem.at[h, u, p, 3],
                   dsem.at[h, u, p], partner)
        if p == 0:
            ca = rcopy(auxall.at[h, u, amine], auxall.at[h, u, amine], sasem.at[h, u, 3], dasem.at[h, u], partner)
            ca.start() if op == "start" else ca.wait_send()
        cx.start() if op == "start" else cx.wait_send()

    def own_full(h, op):
        cx = rcopy(x_ref, xall.at[h, me], ssem.at[h, me, 0, 3], dsem.at[h, me, 0], partner)
        ca = rcopy(aux_ref, auxall.at[h, me], sasem.at[h, me, 3], dasem.at[h, me], partner)
        for cp in (ca, cx):
            if op == "start":
                cp.start()
            elif op == "send":
                cp.wait_send()
            else:
                cp.wait_recv()

    def own_links(h, op, from_input):
        for p in range(2):
            xs = x_ref.at[part(row0, p)] if from_input else None
            xas = aux_ref.at[amine] if from_input else None

            @pl.when(z < 3)
            def _():
                link_send(h, me, p, 0, up, op, xs, xas)

            @pl.when(z > 0)
            def _():
                link_send(h, me, p, 1, down, op, xs, xas)

            link_send(h, me, p, 2, ynbr, op, xs, xas)

    def own_start(h):
        @pl.when(c == h)
        def _():
            own_links(h, "start", True)
            xall[h, me] = x_ref[...]
            auxall[h, me] = aux_ref[...]

        @pl.when(c != h)
        def _():
            own_full(h, "recv")
            own_links(h, "start", False)

    def forwards(h, zz, yy, p, op):
        u = zz * 2 + yy

        @pl.when(yy == y)
        def _():
            @pl.when(jnp.logical_and(zz < z, z < 3))
            def _():
                link_send(h, u, p, 0, up, op)

            @pl.when(jnp.logical_and(zz > z, z > 0))
            def _():
                link_send(h, u, p, 1, down, op)

            if p == 0:
                link_send(h, u, p, 2, ynbr, op)
            else:
                @pl.when(zz != pz)
                def _():
                    link_send(h, u, p, 2, ynbr, op)

        d2d_send(h, u, p, op)

    def alt_forward(h, op):
        u = z * 2 + (1 - y)

        @pl.when(z % 2 == 0)
        def _():
            link_send(h, u, 1, 0, up, op)

        @pl.when(z % 2 == 1)
        def _():
            link_send(h, u, 1, 1, down, op)

    def piece(k):
        along_z = (1 - k % 2) * (1 - k // 6)
        i = k // 2
        first = 1 - (i + 2) // 3
        zi = _z_order(z, i - i // 3)
        zy = first * z + (1 - first) * _z_order(z, (i - 1) * (1 - first))
        zz = along_z * zi + (1 - along_z) * zy
        yy = along_z * y + (1 - along_z) * (1 - y)
        return zz, yy

    def ag_sub(h, k, p):
        zz, yy = piece(k)
        u = zz * 2 + yy
        if p == 0:
            rcopy(auxall.at[h, u, amine], auxall.at[h, u, amine], sasem.at[h, u, 0], lasem.at[h, u],
                  partner).wait_recv()
        rcopy(xall.at[h, u, part(row0, p)], xall.at[h, u, part(row0, p)], ssem.at[h, u, p, 0], lsem.at[h, u, p],
              partner).wait_recv()
        forwards(h, zz, yy, p, "start")

    def d2d_wait(h, k):
        zz, yy = piece(k)
        u = zz * 2 + yy
        aoth = pl.ds(pl.multiple_of((1 - c) * 8, 8), 8)
        rcopy(auxall.at[h, u, aoth], auxall.at[h, u, aoth], sasem.at[h, u, 0], dasem.at[h, u], partner).wait_recv()
        for p in range(2):
            rcopy(xall.at[h, u, part(oth0, p)], xall.at[h, u, part(oth0, p)], ssem.at[h, u, p, 0], dsem.at[h, u, p],
                  partner).wait_recv()
        return u

    def gather(h, u):
        aux = auxall[h, u]
        eg = (lax.broadcasted_iota(jnp.int32, (EL, T), 0) + z * EL).astype(F32)
        hit = jnp.zeros((EL, T), F32)
        gate = jnp.zeros((EL, T), F32)
        for j in range(TOP):
            eq = aux[j:j + 1, :] == eg
            hit = jnp.where(eq, 1.0, hit)
            gate = jnp.where(eq, aux[TOP + j:TOP + j + 1, :], gate)
        before = lax.broadcasted_iota(jnp.int32, (T, T), 0) < lax.broadcasted_iota(jnp.int32, (T, T), 1)
        tri = jnp.where(before, 1.0, 0.0).astype(BF16)
        slot = jnp.dot(hit.astype(BF16), tri, preferred_element_type=F32)
        keep = jnp.logical_and(hit > 0.5, slot < CAP - 0.5)
        slot = jnp.where(keep, slot, -1.0)
        g1 = gate.astype(BF16).astype(F32)
        r1 = gate - g1
        g2 = r1.astype(BF16).astype(F32)
        g3 = r1 - g2
        stack = jnp.concatenate([slot, g1, g2, g3, jnp.zeros((T - 4 * EL, T), F32)], axis=0)
        tab[h, u] = stack.T.astype(BF16)
        pos = lax.broadcasted_iota(jnp.int32, (EL, CAP, T), 1).astype(F32)
        hot = jnp.where(slot[:, None, :] == pos, 1.0, 0.0).reshape(EL * CAP, T).astype(BF16)
        rows = pl.ds(pl.multiple_of(u * CAP, CAP), CAP)
        for n in range(0, d, 512):
            xg = jnp.dot(hot, xall[h, u, :, n:n + 512], preferred_element_type=F32).astype(BF16)
            xe[:, rows, n:n + 512] = xg.reshape(EL, CAP, 512)

    def expert(q):
        e, s = q % EL, q % NS
        c1, c3, c2 = wcopies(q)
        c1.wait()
        c3.wait()
        c2.wait()
        a = jnp.dot(xe[e], w1b[s], preferred_element_type=F32)
        b = jnp.dot(xe[e], w3b[s], preferred_element_type=F32)
        hh = (a * jax.nn.sigmoid(a) * b).astype(BF16)
        for n in range(0, d, 512):
            xe[e, :, n:n + 512] = jnp.dot(hh, w2b[s, :, n:n + 512], preferred_element_type=F32).astype(BF16)

        @pl.when(q + NS < 2 * EL)
        def _():
            for cp in wcopies(q + NS):
                cp.start()

    slots_of = (lax.broadcasted_iota(jnp.int32, (T, EL * CAP), 1) % CAP).astype(F32)

    def dcopy(h, u):
        return rcopy(dstage.at[u], drecv.at[h, u], rd_s.at[h, u], rd_r.at[h, u], partner)

    def sub(p):
        return pl.ds(p * PART, PART)

    def ycopy(h, zz, p):
        return rcopy(ystage.at[zz, sub(p)], yrecv.at[h, zz, sub(p)], ry_s.at[h, zz, p], ry_r.at[h, zz, p], ynbr)

    def zcopy(h, zz, slot, p, dev):
        return rcopy(zstage.at[zz, sub(p)], zrecv.at[h, slot, sub(p)], rz_s.at[h, zz, p], rz_r.at[h, slot, p], dev)

    def acopy(h, dev):
        return rcopy(astage.at[h], arecv.at[h], ra_s.at[h], ra_r.at[h], dev)

    def fcopy():
        return rcopy(fstage, frecv, rf_s, rf_r, partner)

    def combine(h, u):
        tb = jnp.concatenate([tab[h, u, mine], tab[h, u, pl.ds(oth0, HALF)]], axis=0)
        ex = jnp.dot(tb, spread[...], preferred_element_type=F32)
        n0 = EL * CAP
        on = ex[:, :n0] == slots_of
        lhs = jnp.concatenate([jnp.where(on, ex[:, k * n0:(k + 1) * n0], 0.0).astype(BF16) for k in (1, 2, 3)], axis=0)
        rows = pl.ds(pl.multiple_of(u * CAP, CAP), CAP)
        if h == 1:
            dcopy(0, u).wait_send()
        for n in range(0, d, 512):
            yy = xe[:, rows, n:n + 512].reshape(EL * CAP, 512)
            p3 = jnp.dot(lhs, yy, preferred_element_type=F32)
            p = p3[:T] + p3[T:2 * T] + p3[2 * T:]
            pown[u, :, n:n + 512] = p[:HALF]
            dstage[u, :, n:n + 512] = p[HALF:].astype(BF16)
        dcopy(h, u).start()

    def alt_send(h):
        u = pz * 2 + (1 - y)
        dcopy(h, u).wait_recv()
        astage[h] = (pown[u, PART:, :] + drecv[h, u, PART:, :].astype(F32)).astype(BF16)

        @pl.when(z % 2 == 0)
        def _():
            acopy(h, up).start()

        @pl.when(z % 2 == 1)
        def _():
            acopy(h, down).start()

    def fin_y(h, i):
        zz = _r_order(z, i)
        u = zz * 2 + (1 - y)

        @pl.when(zz != pz)
        def _():
            dcopy(h, u).wait_recv()

        if h == 1:
            ycopy(0, zz, 0).wait_send()
        ystage[zz, :PART, :] = (pown[u, :PART, :] + drecv[h, u, :PART, :].astype(F32)).astype(BF16)
        ycopy(h, zz, 0).start()

        @pl.when(zz == z)
        def _():
            acopy(h, up).wait_recv()
            pown[u, PART:, :] = pown[u, PART:, :] + arecv[h].astype(F32)

        @pl.when(zz != pz)
        def _():
            if h == 1:
                ycopy(0, zz, 1).wait_send()
            ystage[zz, PART:, :] = (pown[u, PART:, :] + drecv[h, u, PART:, :].astype(F32)).astype(BF16)
            ycopy(h, zz, 1).start()

    def fin_z(h, i):
        zz = _r_order(z, i)
        u = zz * 2 + y
        dcopy(h, u).wait_recv()
        for p in range(2):
            r = slice(p * PART, (p + 1) * PART)

            def add_y():
                ycopy(h, zz, p).wait_recv()
                pown[u, r, :] = pown[u, r, :] + yrecv[h, zz, r, :].astype(F32)

            if p == 0:
                add_y()
            else:
                pl.when(zz != pz)(add_y)

            @pl.when(jnp.logical_or(jnp.logical_and(zz > z, z > 0), jnp.logical_and(zz < z, z < 3)))
            def _():
                zcopy(h, zz, zz, p, up).wait_recv()
                pown[u, r, :] = pown[u, r, :] + zrecv[h, zz, r, :].astype(F32)

            if h == 1:
                zcopy(0, zz, zz, p, up).wait_send()
            zstage[zz, r, :] = (pown[u, r, :] + drecv[h, u, r, :].astype(F32)).astype(BF16)

            @pl.when(zz == z + 1)
            def _():
                zcopy(h, zz, 4, p, up).start()

            @pl.when(zz > z + 1)
            def _():
                zcopy(h, zz, zz, p, up).start()

            @pl.when(zz < z)
            def _():
                zcopy(h, zz, zz, p, down).start()

    def fin_own(h):
        u = me
        dcopy(h, u).wait_recv()
        for p in range(2):
            r = slice(p * PART, (p + 1) * PART)
            ycopy(h, z, p).wait_recv()
            pown[u, r, :] = pown[u, r, :] + drecv[h, u, r, :].astype(F32) + yrecv[h, z, r, :].astype(F32)

            @pl.when(z < 3)
            def _():
                zcopy(h, z, z, p, up).wait_recv()
                pown[u, r, :] = pown[u, r, :] + zrecv[h, z, r, :].astype(F32)

            @pl.when(z > 0)
            def _():
                zcopy(h, z, 4, p, up).wait_recv()
                pown[u, r, :] = pown[u, r, :] + zrecv[h, 4, r, :].astype(F32)

        @pl.when(c == h)
        def _():
            out_ref[mine, :] = pown[u].astype(BF16)

        @pl.when(c != h)
        def _():
            fstage[...] = pown[u].astype(BF16)
            fcopy().start()

    for h in range(2):
        @pl.when(c == h)
        def _():
            own_full(h, "start")
    own_start(0)
    lane = lax.broadcasted_iota(jnp.int32, (T, 4 * EL * CAP), 1)
    row_id = lax.broadcasted_iota(jnp.int32, (T, 4 * EL * CAP), 0)
    spread[...] = jnp.where(lane // CAP == row_id, 1.0, 0.0).astype(BF16)

    gather(0, me)

    outer = 1 - inner
    steps = (((0, 0, 2), (1, 0, 2), (2, 0, 1)), ((0, 1, 2), (1, 1, 2), (2, 1, 1)),
             ((2, 0, 0), (3, 0, 2), (4, 0, 1)), ((2, 1, 0), (4, 1, 1)),
             ((4, 0, 0), (5, 0, 2)), ((4, 1, 0), (5, 1, 2)), ((6, 0, 2),), ((6, 1, 2), (3, 1, 2)))

    def a_body(it, _):
        for n, todo in enumerate(steps):
            @pl.when(it == n)
            def _():
                for k, p, where in todo:
                    def step():
                        ag_sub(0, k, p)
                    if where == 2:
                        step()
                    else:
                        pl.when(inner == where)(step)

        @pl.when(it == 3 + 2 * outer)
        def _():
            alt_forward(0, "start")
            own_start(1)

        @pl.when(it > 1)
        def _():
            last, late = it // 8, it // 5 - it // 8
            gather(0, d2d_wait(0, (1 - last) * (it - 2 + late) + last * 3))
        return 0

    lax.fori_loop(0, 9, a_body, 0)

    def ffn_a(e, _):
        expert(e)
        for k in range(6):
            for p in range(2):
                if (k, p) == (3, 1):
                    continue
                at = (5, 7)[p] + 4 * (k // 2) - (4 * inner if k in (2, 4) else 0)

                @pl.when(e == at)
                def _():
                    ag_sub(1, k, p)
                    if (k, p) == (4, 1):
                        alt_forward(1, "start")
        return 0

    lax.fori_loop(0, EL, ffn_a, 0)

    def comb_all(h):
        def body(i, _):
            yy = (1 - i // 4) * (1 - y) + (i // 4) * y
            j = i % 4
            j = j + (1 - inner) * (1 - i // 4) * ((j % 3 + 1) // 2) * (3 - 2 * j)
            combine(h, _r_order(z, j) * 2 + yy)

            @pl.when(i == 2)
            def _():
                alt_send(h)

            @pl.when(jnp.logical_and(i > 0, i < 2))
            def _():
                fin_y(h, 0)

            @pl.when(jnp.logical_and(i > 2, i < 6))
            def _():
                fin_y(h, i - 2)
            if h == 0:
                for at, k, p in ((5, 6, 0), (6, 6, 1), (7, 3, 1)):
                    @pl.when(i == at)
                    def _():
                        ag_sub(1, k, p)
            return 0
        lax.fori_loop(0, 8, body, 0)

    comb_all(0)

    def b_body(k, _):
        @pl.when(k == 0)
        def _():
            gather(1, me)

        @pl.when(k > 0)
        def _():
            gather(1, d2d_wait(1, k - 1))
        return 0

    lax.fori_loop(0, 8, b_body, 0)

    def ffn_b(e, _):
        expert(EL + e)
        for i, at in enumerate((2, 4, 8)):
            @pl.when(e == at)
            def _():
                fin_z(0, i)

        @pl.when(e == 14)
        def _():
            fin_own(0)
        return 0

    lax.fori_loop(0, EL, ffn_b, 0)
    comb_all(1)

    def last_z(i, _):
        fin_z(1, i)
        return 0

    lax.fori_loop(0, 3, last_z, 0)
    fin_own(1)

    fcopy().wait_recv()
    out_ref[pl.ds(oth0, HALF), :] = frecv[...]

    fcopy().wait_send()
    for h in range(2):
        @pl.when(c == h)
        def _():
            own_full(h, "send")
        own_links(h, "send", False)
        alt_forward(h, "send")
        acopy(h, up).wait_send()

        def drain(k, _):
            zz, yy = piece(k)
            for p in range(2):
                forwards(h, zz, yy, p, "send")
            return 0
        lax.fori_loop(0, 7, drain, 0)

    def drain_r(i, _):
        zz = _r_order(z, i)
        dcopy(1, zz * 2).wait_send()
        dcopy(1, zz * 2 + 1).wait_send()
        ycopy(1, zz, 0).wait_send()

        @pl.when(zz != pz)
        def _():
            ycopy(1, zz, 1).wait_send()

        @pl.when(i < 3)
        def _():
            zcopy(1, zz, zz, 0, up).wait_send()
            zcopy(1, zz, zz, 1, up).wait_send()
        return 0
    lax.fori_loop(0, 4, drain_r, 0)


def solution(mesh):
    rows = P(("dp", "ep", "tp"), None)

    def local(x, idx, g, w1, w3, w2):
        d = x.shape[1]
        f = w1.shape[2]
        aux = jnp.concatenate([idx.T.astype(F32), g.T], axis=0)
        vm = pl.BlockSpec(memory_space=pltpu.VMEM)
        hbm = pl.BlockSpec(memory_space=pl.ANY)
        dma = pltpu.SemaphoreType.DMA
        return pl.pallas_call(
            _kernel,
            out_shape=jax.ShapeDtypeStruct((T, d), BF16),
            in_specs=[vm, vm, hbm, hbm, hbm],
            out_specs=vm,
            scratch_shapes=[
                pltpu.VMEM((2, UNITS, T, d), BF16),
                pltpu.VMEM((2, UNITS, 2 * TOP, T), F32),
                pltpu.VMEM((EL, ROWS, d), BF16),
                pltpu.VMEM((NS, d, f), BF16),
                pltpu.VMEM((NS, d, f), BF16),
                pltpu.VMEM((NS, f, d), BF16),
                pltpu.VMEM((T, 4 * EL * CAP), BF16),
                pltpu.VMEM((2, UNITS, T, T), BF16),
                pltpu.VMEM((UNITS, HALF, d), F32),
                pltpu.VMEM((UNITS, HALF, d), BF16),
                pltpu.VMEM((2, UNITS, HALF, d), BF16),
                pltpu.VMEM((4, HALF, d), BF16),
                pltpu.VMEM((2, 4, HALF, d), BF16),
                pltpu.VMEM((4, HALF, d), BF16),
                pltpu.VMEM((2, 5, HALF, d), BF16),
                pltpu.VMEM((HALF, d), BF16),
                pltpu.VMEM((HALF, d), BF16),
                pltpu.VMEM((2, PART, d), BF16),
                pltpu.VMEM((2, PART, d), BF16),
                dma((2, UNITS, 2)), dma((2, UNITS)), dma((2, UNITS, 2)), dma((2, UNITS)),
                dma((2, UNITS, 2, 4)), dma((2, UNITS, 4)),
                dma((NS, 3)),
                dma((2, UNITS)), dma((2, UNITS)),
                dma((2, 4, 2)), dma((2, 4, 2)),
                dma((2, 4, 2)), dma((2, 5, 2)),
                dma((2,)), dma((2,)),
                dma, dma,
            ],
            compiler_params=pltpu.CompilerParams(collective_id=0, has_side_effects=True,
                                                 vmem_limit_bytes=67043328),
        )(x, aux, w1, w3, w2)

    return jax.shard_map(local, mesh=mesh,
                         in_specs=(rows, rows, rows, P("ep", None, "tp"), P("ep", None, "tp"), P("ep", "tp", None)),
                         out_specs=rows, check_vma=False)
```
